16 devices in a mesh: dp: 2 (over y, z), sp: 8 (over x, core).
Axes of the slice: x: 4, y: 2, z: 1, core: 2. Of those that a mesh axis runs over, the one named last changes fastest.
The devices are a block of a 4x4x8 slice.
Arguments:
- tokens: bfloat16 [12, 4096, 2048], P('dp', 'sp'), parts along dimension 0
- w_query: bfloat16 [2048, 4096], replicated
- w_key: bfloat16 [2048, 512], replicated
- w_value: bfloat16 [2048, 512], replicated
- w_out: bfloat16 [4096, 2048], replicated
- attn_norm: bfloat16 [2048], replicated
- q_norm: bfloat16 [128], replicated
- k_norm: bfloat16 [128], replicated
Outputs:
- output 1: bfloat16 [12, 4096, 2048], P('dp', 'sp'), parts along dimension 0
- output 2: bfloat16 [12, 4096, 4, 128], P('dp', 'sp'), parts along dimension 0
- output 3: bfloat16 [12, 4096, 4, 128], P('dp', 'sp'), parts along dimension 0
There are 2 independent parts. The reference program is written for one: setup_inputs(seed, part) draws one part's arguments, and reference() takes and returns one part's arrays. A program takes and returns all parts, laid end to end along the dimension named above; an argument that names none is the same for every part.
All inputs are finite; a program needn't handle non-finite values.
Results may differ from the reference program's by a relative error of at most 0.00827115.
Values are sent between devices in bfloat16 or wider.
A program may use at most 768 MiB of HBM per device.

```python
import jax
import jax.numpy as jnp
from jax import lax

BATCH = 6
SEQ_LEN = 4096
D_MODEL = 2048
HEADS = 32
KV_HEADS = 4
HEAD_DIM = 128
EPS = 1e-6
THETA = 1000000.0
Q_BLOCK = min(128, SEQ_LEN)
N_QBLK = SEQ_LEN // Q_BLOCK
GROUP = HEADS // KV_HEADS
SCALE = HEAD_DIM ** -0.5


def rms_norm(values, gain_vec):
    wide_vals = values.astype(jnp.float32)
    inv_rms = lax.rsqrt(jnp.mean(wide_vals * wide_vals, axis=-1, keepdims=True) + EPS)
    return wide_vals * inv_rms * gain_vec.astype(jnp.float32)


def rope_rotate(values, positions):
    half_dim = HEAD_DIM // 2
    inv_freq = THETA ** (-jnp.arange(half_dim, dtype=jnp.float32) * 2.0 / HEAD_DIM)
    angles = positions.astype(jnp.float32)[:, None] * inv_freq[None, :]
    cos_t = jnp.cos(angles)[None, :, None, :]
    sin_t = jnp.sin(angles)[None, :, None, :]
    lo_half = values[..., :half_dim]
    hi_half = values[..., half_dim:]
    return jnp.concatenate([lo_half * cos_t - hi_half * sin_t, hi_half * cos_t + lo_half * sin_t], axis=-1)


def setup_inputs(seed: int = 0, part: int = 0) -> dict:
    part_key = jax.random.fold_in(jax.random.key(seed), part)
    noise_key, walk_key = jax.random.split(part_key, 2)
    shared = jax.random.split(jax.random.key(seed + 1), 7)
    noise_part = 0.5 * jax.random.normal(noise_key, (BATCH, SEQ_LEN, D_MODEL), jnp.float32)
    walk_steps = jax.random.normal(walk_key, (BATCH, SEQ_LEN, D_MODEL), jnp.float32)
    walk_part = jnp.cumsum(walk_steps, axis=1) * (1.5 / SEQ_LEN ** 0.5)
    tokens = (noise_part + walk_part).astype(jnp.bfloat16)

    def make_dense(rng_key, fan_in, fan_out):
        return (jax.random.normal(rng_key, (fan_in, fan_out), jnp.float32) * fan_in ** -0.5).astype(jnp.bfloat16)

    def draw_gain(rng_key, n_elems, center, spread):
        return (center + spread * jax.random.normal(rng_key, (n_elems,), jnp.float32)).astype(jnp.bfloat16)

    return {
        'tokens': tokens,
        'w_query': make_dense(shared[0], D_MODEL, HEADS * HEAD_DIM),
        'w_key': make_dense(shared[1], D_MODEL, KV_HEADS * HEAD_DIM),
        'w_value': make_dense(shared[2], D_MODEL, KV_HEADS * HEAD_DIM),
        'w_out': make_dense(shared[3], HEADS * HEAD_DIM, D_MODEL),
        'attn_norm': draw_gain(shared[4], D_MODEL, 1.0, 0.3),
        'q_norm': draw_gain(shared[5], HEAD_DIM, 1.4, 0.4),
        'k_norm': draw_gain(shared[6], HEAD_DIM, 1.4, 0.4),
    }


def reference(tokens, w_query, w_key, w_value, w_out, attn_norm, q_norm, k_norm):
    hidden = rms_norm(tokens, attn_norm).astype(jnp.bfloat16).reshape(BATCH * SEQ_LEN, D_MODEL)
    q_proj = jnp.dot(hidden, w_query, preferred_element_type=jnp.float32).astype(jnp.bfloat16).reshape(BATCH, SEQ_LEN, HEADS, HEAD_DIM)
    k_proj = jnp.dot(hidden, w_key, preferred_element_type=jnp.float32).astype(jnp.bfloat16).reshape(BATCH, SEQ_LEN, KV_HEADS, HEAD_DIM)
    v_proj = jnp.dot(hidden, w_value, preferred_element_type=jnp.float32).astype(jnp.bfloat16).reshape(BATCH, SEQ_LEN, KV_HEADS, HEAD_DIM)
    positions = jnp.arange(SEQ_LEN)
    q_rot = rope_rotate(rms_norm(q_proj, q_norm), positions).astype(jnp.bfloat16)
    k_rot = rope_rotate(rms_norm(k_proj, k_norm), positions).astype(jnp.bfloat16)
    key_pos = jnp.arange(SEQ_LEN)
    row_ids = jnp.arange(Q_BLOCK)

    def one_seq(seq_args):
        q_seq, k_seq, v_seq = seq_args
        k_wide = k_seq.astype(jnp.float32)
        v_wide = v_seq.astype(jnp.float32)
        q_blocks = q_seq.reshape(N_QBLK, Q_BLOCK, KV_HEADS, GROUP, HEAD_DIM)

        def one_block(blk_args):
            q_blk, blk_idx = blk_args
            scores = jnp.einsum('qkgd,skd->kgqs', q_blk.astype(jnp.float32), k_wide) * SCALE
            allowed = key_pos[None, :] <= (blk_idx * Q_BLOCK + row_ids)[:, None]
            scores = jnp.where(allowed[None, None], scores, -jnp.inf)
            probs_blk = jax.nn.softmax(scores, axis=-1)
            return jnp.einsum('kgqs,skd->qkgd', probs_blk, v_wide).astype(jnp.bfloat16)

        attn_blocks = lax.map(one_block, (q_blocks, jnp.arange(N_QBLK)))
        return attn_blocks.reshape(SEQ_LEN, HEADS * HEAD_DIM)

    attn_out = lax.map(one_seq, (q_rot, k_rot, v_proj))
    proj_out = jnp.dot(attn_out.reshape(BATCH * SEQ_LEN, HEADS * HEAD_DIM), w_out, preferred_element_type=jnp.float32)
    output = (tokens.astype(jnp.float32) + proj_out.reshape(BATCH, SEQ_LEN, D_MODEL)).astype(jnp.bfloat16)
    return (output, k_rot, v_proj)
```

```python
import functools
import math

import jax
import jax.numpy as jnp
import numpy as np
from jax import lax
from jax.experimental import pallas as pl
from jax.experimental.pallas import tpu as pltpu
from jax.sharding import PartitionSpec as P

EPS = 1e-6
THETA = 1000000.0
HD = 128
T = 64
VMEM_LIMIT = 60 * 1024 * 1024
Q_COLS = 512
DIAG_STEP = 256
TILE_COST, ITEM_COST = 15.0, 9.5


def split_work(n_sp, n_tiles):
    moved = [0] * n_sp
    for d in range((n_sp + 1) // 2, n_sp):
        low = n_sp - 1 - d
        heavy, light = TILE_COST + ITEM_COST * (d + 1), TILE_COST + ITEM_COST * (low + 1)
        moved[d] = min(range(n_tiles // 2 + 1), key=lambda k: max(n_tiles * heavy - k * heavy, n_tiles * light + k * heavy))
    return moved


def normed(x_ref, gain_ref):
    p, r, d = x_ref.shape
    x = x_ref[...].reshape(p * r, d).astype(jnp.float32)
    inv = lax.rsqrt(jnp.mean(x * x, axis=-1, keepdims=True) + EPS)
    return (x * inv * gain_ref[...].astype(jnp.float32)).astype(jnp.bfloat16)


def head_norm_rope(y, gain, cos, sin, n_rep):
    inv = lax.rsqrt(jnp.mean(y * y, axis=-1, keepdims=True) + EPS)
    y = y * inv * gain
    rolled = pltpu.roll(y, HD // 2, 1)
    r = cos.shape[0]
    y, rolled = y.reshape(n_rep, r, HD), rolled.reshape(n_rep, r, HD)
    return (y * cos[None] + rolled * sin[None]).astype(jnp.bfloat16)


def kv_kernel(x_ref, wk_ref, wv_ref, g_ref, kg_ref, cos_ref, sin_ref, k_ref, v_ref, pack_ref):
    n_p, r, _ = x_ref.shape
    i = pl.program_id(0)
    h = normed(x_ref, g_ref)
    k = jnp.dot(h, wk_ref[...], preferred_element_type=jnp.float32).astype(jnp.bfloat16).astype(jnp.float32)
    v = jnp.dot(h, wv_ref[...], preferred_element_type=jnp.float32).astype(jnp.bfloat16)
    gain = kg_ref[...].astype(jnp.float32)
    cos, sin = cos_ref[...], sin_ref[...]
    rows = pl.ds(pl.multiple_of(i * r, r), r)
    v_ref[...] = v.reshape(v_ref.shape)
    for p in range(n_p):
        pack_ref[p, 1, :, rows] = v[p * r:(p + 1) * r].T
    for j in range(k.shape[1] // HD):
        y = head_norm_rope(k[:, j * HD:(j + 1) * HD], gain, cos, sin, n_p)
        k_ref[:, :, j * HD:(j + 1) * HD] = y
        pack_ref[:, 0, rows, j * HD:(j + 1) * HD] = y


def kv_project(x, w_key, w_value, gain, k_gain, cos, sin):
    n_p, rows, d = x.shape
    w = w_key.shape[1]
    r = min(128, rows)
    whole = lambda shape: pl.BlockSpec(shape, lambda i: (0,) * len(shape))
    return pl.pallas_call(
        kv_kernel,
        out_shape=(
            jax.ShapeDtypeStruct((n_p, rows, w), x.dtype),
            jax.ShapeDtypeStruct((n_p, rows, w), x.dtype),
            jax.ShapeDtypeStruct((n_p, 2, rows, w), x.dtype),
        ),
        grid=(rows // r,),
        in_specs=[
            pl.BlockSpec((n_p, r, d), lambda i: (0, i, 0)),
            whole((d, w)), whole((d, w)), whole((1, d)), whole((1, HD)),
            pl.BlockSpec((r, HD), lambda i: (i, 0)), pl.BlockSpec((r, HD), lambda i: (i, 0)),
        ],
        out_specs=(
            pl.BlockSpec((n_p, r, w), lambda i: (0, i, 0)),
            pl.BlockSpec((n_p, r, w), lambda i: (0, i, 0)),
            whole((n_p, 2, rows, w)),
        ),
        compiler_params=pltpu.CompilerParams(dimension_semantics=("arbitrary",), vmem_limit_bytes=VMEM_LIMIT),
        cost_estimate=pl.CostEstimate(flops=4 * n_p * rows * d * w, bytes_accessed=8 * n_p * rows * d, transcendentals=0),
        name="kv_proj",
    )(x, w_key, w_value, gain, k_gain, cos, sin)


def q_kernel(first_tile, nc, valid_ref, x_ref, w_ref, g_ref, qg_ref, cos_ref, sin_ref, *rest):
    q_ref, h_scr, y_scr = rest[-3:]
    n_p, _, _ = x_ref.shape

    @pl.when(valid_ref[first_tile + pl.program_id(0)] == 1)
    def _():
        h_scr[...] = normed(x_ref, g_ref)
        gain = qg_ref[...].astype(jnp.float32) * (math.log2(math.e) / math.sqrt(HD))
        cos, sin = cos_ref[...], sin_ref[...]
        n_chunks = w_ref.shape[1] // nc

        def project(n):
            cols = pl.ds(pl.multiple_of(n * nc, nc), nc)
            y_scr[...] = jnp.dot(h_scr[...], w_ref[:, cols], preferred_element_type=jnp.float32).astype(jnp.bfloat16)

        def finish(n):
            for j in range(nc // HD):
                y = head_norm_rope(y_scr[:, j * HD:(j + 1) * HD].astype(jnp.float32), gain, cos, sin, n_p)
                q_ref[:, :, pl.ds(pl.multiple_of(n * nc + j * HD, HD), HD)] = y

        def step(n, _):
            finish(n)
            project(n + 1)
            return 0

        project(0)
        lax.fori_loop(0, n_chunks - 1, step, 0)
        finish(n_chunks - 1)


def q_project(x, w_query, gain, q_gain, cos, sin, valid, first_tile, total_tiles, into):
    n_p, rows, d = x.shape
    w = w_query.shape[1]
    whole = lambda shape: pl.BlockSpec(shape, lambda i, *_: (0,) * len(shape))
    args = [valid, x, w_query, gain, q_gain, cos, sin]
    specs = [
        pl.BlockSpec((n_p, T, d), lambda i, *_: (0, i, 0)),
        pl.BlockSpec((d, w), lambda i, *_: (0, 0), pipeline_mode=pl.Buffered(1)),
        whole((1, d)), whole((1, HD)),
        pl.BlockSpec((T, HD), lambda i, *_: (i + first_tile, 0)), pl.BlockSpec((T, HD), lambda i, *_: (i + first_tile, 0)),
    ]
    alias = {}
    if into is not None:
        args.append(into)
        specs.append(pl.BlockSpec(memory_space=pl.ANY))
        alias = {7: 0}
    return pl.pallas_call(
        functools.partial(q_kernel, first_tile, Q_COLS),
        out_shape=jax.ShapeDtypeStruct((n_p, total_tiles * T, w), x.dtype),
        grid_spec=pltpu.PrefetchScalarGridSpec(
            num_scalar_prefetch=1,
            grid=(rows // T,),
            in_specs=specs,
            out_specs=pl.BlockSpec((n_p, T, w), lambda i, *_: (0, i + first_tile, 0)),
            scratch_shapes=[pltpu.VMEM((n_p * T, d), x.dtype), pltpu.VMEM((n_p * T, Q_COLS), x.dtype)],
        ),
        input_output_aliases=alias,
        compiler_params=pltpu.CompilerParams(dimension_semantics=("arbitrary",), vmem_limit_bytes=VMEM_LIMIT),
        cost_estimate=pl.CostEstimate(flops=2 * n_p * rows * d * w, bytes_accessed=2 * n_p * rows * (d + w), transcendentals=0),
        name="q_proj",
    )(*args)


def attn_kernel(n_tiles, grp, bk, ext_step, hp, ck, info_ref, q_ref, k_ref, v_ref, after_ref, o_ref, q_scr, s_scr, bm_scr, m_scr, l_scr, acc_scr):
    del after_ref
    n = grp * T
    base = 2 * n_tiles + 2
    m_items = (info_ref.shape[0] - base) // 4

    def tile(i): return info_ref[base + i]

    def blk(i): return info_ref[base + m_items + i]

    def first(i): return info_ref[base + 2 * m_items + i]

    def diag(i): return info_ref[base + 3 * m_items + i]

    @pl.when((pl.program_id(0) == 0) & (pl.program_id(1) == 0))
    def _():
        l_scr[...] = jnp.zeros_like(l_scr)
        acc_scr[...] = jnp.zeros_like(acc_scr)
        m_scr[...] = jnp.zeros_like(m_scr)

    for h in range(hp):
        for t in range(n_tiles):
            for j in range(grp):
                q_scr[h, t, j * T:(j + 1) * T, :] = q_ref[0, t * T:(t + 1) * T, (h * grp + j) * HD:(h * grp + j + 1) * HD]

    def fold(x, op):
        return op(x.reshape(x.shape[0] // 8, 8, n), axis=0)

    def qk_chunk(i, h, r):
        s = lax.dot_general(k_ref[blk(i), r * ck:(r + 1) * ck, h * HD:(h + 1) * HD], q_scr[h, tile(i)], (((1,), (1,)), ((), ())), preferred_element_type=jnp.float32)
        s_scr[h, r * ck:(r + 1) * ck, :] = s
        return fold(s, jnp.max)

    def masked_chunk(i, h, r, ext):
        s = s_scr[h, r * ck:r * ck + ext, :]
        off = info_ref[n_tiles + tile(i)] - blk(i) * bk - r * ck
        row = lax.broadcasted_iota(jnp.int32, (ext, n), 0)
        col = lax.broadcasted_iota(jnp.int32, (ext, n), 1) & (T - 1)
        return jnp.where(row - col <= off, s, -jnp.inf)

    def body(i, ext, masked):
        b = blk(i)
        fresh = first(i) == 1
        for h in range(hp):
            if masked:
                bm = jnp.full((8, n), -jnp.inf, jnp.float32)
                for r in range(bk // ck):
                    e = min(ck, ext - r * ck)
                    if e <= 0:
                        continue
                    if r * ck + e > ext - ext_step:
                        sm = masked_chunk(i, h, r, e)
                        s_scr[h, r * ck:r * ck + e, :] = sm
                    else:
                        sm = s_scr[h, r * ck:r * ck + e, :]
                    bm = jnp.maximum(bm, fold(sm, jnp.max))
            else:
                bm = bm_scr[h]
            m_old = jnp.where(fresh, -jnp.inf, m_scr[h])
            m_new = jnp.maximum(m_old, jnp.max(bm, axis=0, keepdims=True))
            m_scr[h] = m_new
            alpha = jnp.exp2(m_old - m_new)
            l = l_scr[h] * alpha
            pv = None
            bm_next = None
            for r in range(bk // ck):
                e = min(ck, ext - r * ck)
                if e > 0:
                    p = jnp.exp2(s_scr[h, r * ck:r * ck + e, :] - m_new)
                    l = l + fold(p, jnp.sum)
                    d = jnp.dot(v_ref[b, h * HD:(h + 1) * HD, r * ck:r * ck + e], p.astype(jnp.bfloat16), preferred_element_type=jnp.float32)
                    pv = d if pv is None else pv + d
                x = qk_chunk(i + 1, h, r)
                bm_next = x if bm_next is None else jnp.maximum(bm_next, x)
            l_scr[h] = l
            bm_scr[h] = bm_next
            acc_scr[h] = acc_scr[h] * alpha + pv

    def finish(i):
        t = tile(i)
        for h in range(hp):
            inv = 1.0 / jnp.sum(l_scr[h], axis=0, keepdims=True)
            o = (acc_scr[h] * inv).T.astype(o_ref.dtype)
            for j in range(grp):
                o_ref[0, pl.ds(pl.multiple_of(t * T, T), T), (h * grp + j) * HD:(h * grp + j + 1) * HD] = o[j * T:(j + 1) * T]

    cnt = info_ref[2 * n_tiles]

    @pl.when(cnt > 0)
    def _():
        for h in range(hp):
            bm = None
            for r in range(bk // ck):
                x = qk_chunk(0, h, r)
                bm = x if bm is None else jnp.maximum(bm, x)
            bm_scr[h] = bm

        def step(i, _):
            d = diag(i)

            @pl.when(d == 0)
            def _():
                body(i, bk, False)

            for e in range(bk // ext_step):
                @pl.when(d == e + 1)
                def _():
                    body(i, (e + 1) * ext_step, True)
                    finish(i)
            return 0

        lax.fori_loop(0, cnt, step, 0)


def make_info(n_sp, seq_loc, moved, ext_step):
    n_tiles, spare = seq_loc // T, max(moved)
    rows = []
    for me in range(n_sp):
        other = n_sp - 1 - me
        pos = [me * seq_loc + t * T for t in range(n_tiles)]
        pos += [(other + 1) * seq_loc - (spare - t) * T for t in range(spare)]
        valid = [t < n_tiles - moved[me] for t in range(n_tiles)] + [t >= spare - moved[other] for t in range(spare)]
        items = []
        for t, p in enumerate(pos):
            if valid[t]:
                last = p // seq_loc
                for b in range(last + 1):
                    items.append((t, b, int(b == 0), (p - last * seq_loc) // ext_step + 1 if b == last else 0))
        rows.append(([int(v) for v in valid] + pos + [len(items), int(moved[other] > 0)], items))
    m = max(len(items) for _, items in rows) + 1
    out = []
    for head, items in rows:
        items = items + [(0, 0, 0, 0)] * (m - len(items))
        out.append(head + [item[k] for k in range(4) for item in items])
    return np.asarray(out, np.int32)


def attention(q, kv, info, after, first_prompt, n_kv, hp=4, ck=256):
    _, rows, width = q.shape
    grp = width // HD // n_kv
    n_dev, nb, _, bk, _ = kv.shape
    n_tiles = rows // T
    n = grp * T
    block = pl.BlockSpec((1, rows, hp * grp * HD), lambda p, h, *_: (p + first_prompt, 0, h))
    flops = 2 * 4 * nb * rows * width * n_dev * bk // 2
    return pl.pallas_call(
        functools.partial(attn_kernel, n_tiles, grp, bk, DIAG_STEP, hp, ck),
        out_shape=jax.ShapeDtypeStruct((nb, rows, width), q.dtype),
        grid_spec=pltpu.PrefetchScalarGridSpec(
            num_scalar_prefetch=1,
            grid=(nb, n_kv // hp),
            in_specs=[
                block,
                pl.BlockSpec((n_dev, None, None, bk, hp * HD), lambda p, h, *_: (0, p, 0, 0, h)),
                pl.BlockSpec((n_dev, None, None, hp * HD, bk), lambda p, h, *_: (0, p, 1, h, 0)),
                pl.BlockSpec(memory_space=pl.ANY),
            ],
            out_specs=pl.BlockSpec((1, rows, hp * grp * HD), lambda p, h, *_: (p, 0, h)),
            scratch_shapes=[
                pltpu.VMEM((hp, n_tiles, n, HD), q.dtype),
                pltpu.VMEM((hp, bk, n), jnp.float32),
                pltpu.VMEM((hp, 8, n), jnp.float32),
                pltpu.VMEM((hp, 1, n), jnp.float32),
                pltpu.VMEM((hp, 8, n), jnp.float32),
                pltpu.VMEM((hp, HD, n), jnp.float32),
            ],
        ),
        compiler_params=pltpu.CompilerParams(dimension_semantics=("arbitrary", "arbitrary"), vmem_limit_bytes=VMEM_LIMIT),
        cost_estimate=pl.CostEstimate(flops=flops, bytes_accessed=4 * nb * rows * width, transcendentals=0),
        name="attn",
    )(info, q, kv, kv, after)


def out_moved_kernel(flag, info_ref, o_ref, w_ref, x_ref, y_ref):
    @pl.when(info_ref[flag] == 1)
    def _():
        n_p, r, w = o_ref.shape
        y = jnp.dot(o_ref[...].reshape(n_p * r, w), w_ref[...], preferred_element_type=jnp.float32)
        y_ref[...] = (x_ref[...].astype(jnp.float32) + y.reshape(n_p, r, -1)).astype(y_ref.dtype)


def out_moved(o, w_out, x, info, first_prompt):
    nb, all_rows, w = o.shape
    _, rows, d = x.shape
    first = all_rows - rows
    nc = min(512, d)
    return pl.pallas_call(
        functools.partial(out_moved_kernel, 2 * all_rows // T + 1),
        out_shape=jax.ShapeDtypeStruct((nb, rows, d), x.dtype),
        grid_spec=pltpu.PrefetchScalarGridSpec(
            num_scalar_prefetch=1,
            grid=(d // nc,),
            in_specs=[
                pl.BlockSpec((pl.Element(nb), pl.Element(rows), pl.Element(w)), lambda i, *_: (0, first, 0)),
                pl.BlockSpec((w, nc), lambda i, *_: (0, i)),
                pl.BlockSpec((pl.Element(nb), pl.Element(rows), pl.Element(nc)), lambda i, *_: (first_prompt, 0, i * nc)),
            ],
            out_specs=pl.BlockSpec((nb, rows, nc), lambda i, *_: (0, 0, i)),
        ),
        compiler_params=pltpu.CompilerParams(dimension_semantics=("arbitrary",), vmem_limit_bytes=VMEM_LIMIT),
        cost_estimate=pl.CostEstimate(flops=2 * nb * rows * d * w, bytes_accessed=2 * w * d, transcendentals=0),
        name="out_moved",
    )(info, o, w_out, x)


def out_kernel(n_g, nc, valid_ref, *refs):
    o_refs, (w_ref, x_ref, y_ref, o_scr) = refs[:n_g], refs[n_g:]

    @pl.when(valid_ref[pl.program_id(0)] == 1)
    def _():
        n_p, r, _ = x_ref.shape
        at = 0
        for o_ref in o_refs:
            nb, _, w = o_ref.shape
            o_scr[at:at + nb * r, :] = o_ref[...].reshape(nb * r, w)
            at += nb * r

        def chunk(n, _):
            cols = pl.ds(pl.multiple_of(n * nc, nc), nc)
            y = jnp.dot(o_scr[...], w_ref[:, cols], preferred_element_type=jnp.float32)
            y_ref[:, :, cols] = (x_ref[:, :, cols].astype(jnp.float32) + y.reshape(n_p, r, nc)).astype(y_ref.dtype)
            return 0

        lax.fori_loop(0, w_ref.shape[1] // nc, chunk, 0)


def out_local(o_parts, w_out, x, valid):
    n_p, rows, d = x.shape
    w = o_parts[0].shape[2]
    n_g = len(o_parts)
    return pl.pallas_call(
        functools.partial(out_kernel, n_g, 512),
        out_shape=jax.ShapeDtypeStruct(x.shape, x.dtype),
        grid_spec=pltpu.PrefetchScalarGridSpec(
            num_scalar_prefetch=1,
            grid=(rows // T,),
            in_specs=[pl.BlockSpec((o.shape[0], T, w), lambda i, *_: (0, i, 0)) for o in o_parts] + [
                pl.BlockSpec((w, d), lambda i, *_: (0, 0), pipeline_mode=pl.Buffered(1)),
                pl.BlockSpec((n_p, T, d), lambda i, *_: (0, i, 0)),
            ],
            out_specs=pl.BlockSpec((n_p, T, d), lambda i, *_: (0, i, 0)),
            scratch_shapes=[pltpu.VMEM((n_p * T, w), x.dtype)],
        ),
        compiler_params=pltpu.CompilerParams(dimension_semantics=("arbitrary",), vmem_limit_bytes=VMEM_LIMIT),
        cost_estimate=pl.CostEstimate(flops=2 * n_p * rows * d * w, bytes_accessed=2 * n_p * rows * (d + w), transcendentals=0),
        name="out_local",
    )(valid, *o_parts, w_out, x)


def merge_kernel(valid_ref, first, n_g, *refs):
    y_refs, (cur_ref, out_ref) = refs[:n_g], refs[n_g:]
    kept = valid_ref[first + pl.program_id(0)] == 1

    @pl.when(kept)
    def _():
        out_ref[...] = cur_ref[...]

    @pl.when(jnp.logical_not(kept))
    def _():
        at = 0
        for y_ref in y_refs:
            out_ref[at:at + y_ref.shape[0]] = y_ref[...]
            at += y_ref.shape[0]


def merge(returned, out, valid):
    n_p, rows, d = out.shape
    back = returned[0].shape[1]
    n_g, first = len(returned), (rows - back) // T
    block = pl.BlockSpec((n_p, T, d), lambda i, *_: (0, i + first, 0))
    return pl.pallas_call(
        lambda valid_ref, *refs: merge_kernel(valid_ref, first, n_g, *refs),
        out_shape=jax.ShapeDtypeStruct(out.shape, out.dtype),
        grid_spec=pltpu.PrefetchScalarGridSpec(
            num_scalar_prefetch=1,
            grid=(back // T,),
            in_specs=[pl.BlockSpec((y.shape[0], T, d), lambda i, *_: (0, i, 0)) for y in returned] + [block],
            out_specs=block,
        ),
        input_output_aliases={1 + n_g: 0},
        compiler_params=pltpu.CompilerParams(dimension_semantics=("arbitrary",), vmem_limit_bytes=VMEM_LIMIT),
        name="merge",
    )(valid, *returned, out)


def rotary_tables(positions):
    half = HD // 2
    inv_freq = THETA ** (-jnp.arange(half, dtype=jnp.float32) * 2.0 / HD)
    angles = positions.astype(jnp.float32)[:, None] * inv_freq[None, :]
    cos, sin = jnp.cos(angles), jnp.sin(angles)
    return jnp.concatenate([cos, cos], axis=-1), jnp.concatenate([-sin, sin], axis=-1)


def solution(mesh):
    n_sp = mesh.shape["sp"]

    def block(tokens, w_query, w_key, w_value, w_out, attn_norm, q_norm, k_norm):
        n_p, seq_loc, _ = tokens.shape
        n_kv = w_key.shape[1] // HD
        n_tiles = seq_loc // T
        sizes = []
        while sum(sizes) < n_p:
            sizes.append(min(len(sizes) + 1, n_p - sum(sizes)))
        table = split_work(n_sp, n_tiles)
        spare = max(table)
        me = lax.axis_index("sp")
        gain, q_gain, k_gain = attn_norm.reshape(1, -1), q_norm.reshape(1, -1), k_norm.reshape(1, -1)

        away = [(d, n_sp - 1 - d) for d in range(n_sp) if table[d]]
        x_moved = lax.ppermute(tokens[:, seq_loc - spare * T:, :], "sp", away)

        starts = jnp.concatenate([
            me * seq_loc + jnp.arange(n_tiles) * T,
            (n_sp - me) * seq_loc - spare * T + jnp.arange(spare) * T,
        ])
        cos, sin = rotary_tables((starts[:, None] + jnp.arange(T)[None, :]).reshape(-1))
        info = jnp.asarray(make_info(n_sp, seq_loc, table, DIAG_STEP))[me]

        k, v, pack = kv_project(tokens, w_key, w_value, gain, k_gain, cos, sin)
        kv, at = [], 0
        for s in sizes:
            kv.append(lax.all_gather(pack[at:at + s], "sp"))
            at += s
        total = n_tiles + spare
        q = q_project(tokens, w_query, gain, q_gain, cos, sin, info, 0, total, None)
        q = q_project(x_moved, w_query, gain, q_gain, cos, sin, info, n_tiles, total, q)
        o_parts, returned, at, after = [], [], 0, q
        for s, kv_g in zip(sizes, kv):
            o = attention(q, kv_g, info, after, at, n_kv)
            after = out_moved(o, w_out, x_moved, info, at)
            returned.append(lax.ppermute(after, "sp", [(b, a) for a, b in away]))
            o_parts.append(o)
            at += s
        out = out_local(o_parts, w_out, tokens, info)
        out = merge(returned, out, info)
        return out, k.reshape(n_p, seq_loc, n_kv, HD), v.reshape(n_p, seq_loc, n_kv, HD)

    rows, flat = P("dp", "sp", None), P(None, None)
    cache = P("dp", "sp", None, None)
    return jax.shard_map(
        block,
        mesh=mesh,
        in_specs=(rows, flat, flat, flat, flat, P(None), P(None), P(None)),
        out_specs=(rows, cache, cache),
        check_vma=False,
    )
```

```python
import functools
import math

import jax
import jax.numpy as jnp
import numpy as np
from jax import lax
from jax.experimental import pallas as pl
from jax.experimental.pallas import tpu as pltpu
from jax.sharding import PartitionSpec as P

EPS = 1e-6
THETA = 1000000.0
HD = 128
T = 64
VMEM_LIMIT = 60 * 1024 * 1024
Q_COLS = 512
DIAG_STEP = 256
TILE_COST, TAKEN_COST, ITEM_COST = 17.0, 25.0, 7.5


def split_work(n_sp, n_tiles):
    moved = [0] * n_sp
    for d in range((n_sp + 1) // 2, n_sp):
        low = n_sp - 1 - d
        high, small = ITEM_COST * (d + 1), ITEM_COST * (low + 1)
        moved[d] = min(
            range(n_tiles // 2 + 1),
            key=lambda k: max((n_tiles - k) * (TILE_COST + high), n_tiles * (TILE_COST + small) + k * (TAKEN_COST + high)),
        )
    return moved


def normed(x_ref, gain_ref):
    p, r, d = x_ref.shape
    x = x_ref[...].reshape(p * r, d).astype(jnp.float32)
    inv = lax.rsqrt(jnp.mean(x * x, axis=-1, keepdims=True) + EPS)
    return (x * inv * gain_ref[...].astype(jnp.float32)).astype(jnp.bfloat16)


def head_norm_rope(y, gain, cos, sin, n_rep):
    inv = lax.rsqrt(jnp.mean(y * y, axis=-1, keepdims=True) + EPS)
    y = y * inv * gain
    rolled = pltpu.roll(y, HD // 2, 1)
    r = cos.shape[0]
    y, rolled = y.reshape(n_rep, r, HD), rolled.reshape(n_rep, r, HD)
    return (y * cos[None] + rolled * sin[None]).astype(jnp.bfloat16)


def kv_kernel(sizes, x_ref, wk_ref, wv_ref, g_ref, kg_ref, cos_ref, sin_ref, k_ref, v_ref, h_ref, *pack_refs):
    n_p, r, d = x_ref.shape
    i = pl.program_id(0)
    h = normed(x_ref, g_ref)
    h_ref[...] = h.reshape(n_p, r, d)
    k = jnp.dot(h, wk_ref[...], preferred_element_type=jnp.float32).astype(jnp.bfloat16).astype(jnp.float32)
    v = jnp.dot(h, wv_ref[...], preferred_element_type=jnp.float32).astype(jnp.bfloat16)
    gain = kg_ref[...].astype(jnp.float32)
    cos, sin = cos_ref[...], sin_ref[...]
    rows = pl.ds(pl.multiple_of(i * r, r), r)
    v_ref[...] = v.reshape(v_ref.shape)
    at = 0
    for size, pack_ref in zip(sizes, pack_refs):
        for p in range(size):
            pack_ref[p, 1, :, rows] = v[(at + p) * r:(at + p + 1) * r].T
        at += size
    for j in range(k.shape[1] // HD):
        cols = slice(j * HD, (j + 1) * HD)
        y = head_norm_rope(k[:, cols], gain, cos, sin, n_p)
        k_ref[:, :, cols] = y
        at = 0
        for size, pack_ref in zip(sizes, pack_refs):
            pack_ref[:, 0, rows, cols] = y[at:at + size]
            at += size


def kv_project(x, w_key, w_value, gain, k_gain, cos, sin, sizes):
    n_p, rows, d = x.shape
    w = w_key.shape[1]
    r = min(128, rows)
    whole = lambda shape: pl.BlockSpec(shape, lambda i: (0,) * len(shape))
    cut = lambda cols: pl.BlockSpec((n_p, r, cols), lambda i: (0, i, 0))
    packs = [(s, 2, rows, w) for s in sizes]
    return pl.pallas_call(
        functools.partial(kv_kernel, sizes),
        out_shape=[jax.ShapeDtypeStruct(s, x.dtype) for s in [(n_p, rows, w)] * 2 + [(n_p, rows, d)] + packs],
        grid=(rows // r,),
        in_specs=[
            cut(d), whole((d, w)), whole((d, w)), whole((1, d)), whole((1, HD)),
            pl.BlockSpec((r, HD), lambda i: (i, 0)), pl.BlockSpec((r, HD), lambda i: (i, 0)),
        ],
        out_specs=[cut(w), cut(w), cut(d)] + [whole(s) for s in packs],
        compiler_params=pltpu.CompilerParams(dimension_semantics=("arbitrary",), vmem_limit_bytes=VMEM_LIMIT),
        cost_estimate=pl.CostEstimate(flops=4 * n_p * rows * d * w, bytes_accessed=8 * n_p * rows * d, transcendentals=0),
        name="kv_proj",
    )(x, w_key, w_value, gain, k_gain, cos, sin)


def q_kernel(nc, is_normed, step_of, info_ref, x_ref, w_ref, g_ref, qg_ref, cos_ref, sin_ref, after_ref, q_ref, h_scr, y_scr, w_scr, sem):
    n_p, r, d = x_ref.shape
    i = pl.program_id(0)
    begin, first_tile = step_of(info_ref)
    n_chunks = w_ref.shape[1] // nc

    def cols(n):
        return pl.ds(pl.multiple_of(n * nc, nc), nc)

    def load(n):
        return pltpu.make_async_copy(w_ref.at[:, cols(n)], w_scr.at[:, cols(n)], sem.at[n])

    @pl.when((info_ref[first_tile + i] == 1) & (i >= begin))
    def _():
        @pl.when(i == begin)
        def _():
            for n in range(n_chunks):
                load(n).start()

        h_scr[...] = x_ref[...].reshape(n_p * r, d) if is_normed else normed(x_ref, g_ref)
        gain = qg_ref[...].astype(jnp.float32) * (math.log2(math.e) / math.sqrt(HD))
        cos, sin = cos_ref[...], sin_ref[...]

        def arrived(n):
            @pl.when(i == begin)
            def _():
                load(n).wait()

        def project(n):
            y_scr[...] = jnp.dot(h_scr[...], w_scr[:, cols(n)], preferred_element_type=jnp.float32).astype(jnp.bfloat16)

        def finish(n):
            for j in range(nc // HD):
                y = head_norm_rope(y_scr[:, j * HD:(j + 1) * HD].astype(jnp.float32), gain, cos, sin, n_p)
                q_ref[:, :, pl.ds(pl.multiple_of(n * nc + j * HD, HD), HD)] = y

        def step(n, _):
            arrived(n + 1)
            finish(n)
            project(n + 1)
            return 0

        arrived(0)
        project(0)
        lax.fori_loop(0, n_chunks - 1, step, 0)
        finish(n_chunks - 1)


def q_project(x, w_query, gain, q_gain, cos, sin, info, first_tile, total_tiles, is_normed, after):
    n_p, rows, d = x.shape
    w = w_query.shape[1]
    n_tiles = rows // T
    begin = lambda info: n_tiles - info[2 * total_tiles + 2] if first_tile else 0
    local = lambda i, info: jnp.minimum(jnp.maximum(i, begin(info)), n_tiles - 1)
    whole = lambda shape: pl.BlockSpec(shape, lambda i, info: (0,) * len(shape))
    table = pl.BlockSpec((T, HD), lambda i, info: (local(i, info) + first_tile, 0))
    nc = Q_COLS
    return pl.pallas_call(
        functools.partial(q_kernel, nc, is_normed, lambda info: (begin(info), first_tile)),
        out_shape=jax.ShapeDtypeStruct((n_p, rows, w), x.dtype),
        grid_spec=pltpu.PrefetchScalarGridSpec(
            num_scalar_prefetch=1,
            grid=(n_tiles,),
            in_specs=[
                pl.BlockSpec((n_p, T, d), lambda i, info: (0, local(i, info), 0)),
                pl.BlockSpec(memory_space=pl.ANY),
                whole((1, d)), whole((1, HD)), table, table,
                pl.BlockSpec(memory_space=pl.ANY),
            ],
            out_specs=pl.BlockSpec((n_p, T, w), lambda i, info: (0, local(i, info), 0)),
            scratch_shapes=[
                pltpu.VMEM((n_p * T, d), x.dtype), pltpu.VMEM((n_p * T, nc), x.dtype),
                pltpu.VMEM((d, w), x.dtype), pltpu.SemaphoreType.DMA((w // nc,)),
            ],
        ),
        compiler_params=pltpu.CompilerParams(dimension_semantics=("arbitrary",), vmem_limit_bytes=VMEM_LIMIT),
        cost_estimate=pl.CostEstimate(flops=2 * n_p * rows * d * w, bytes_accessed=2 * n_p * rows * (d + w), transcendentals=0),
        name="q_proj",
    )(info, x, w_query, gain, q_gain, cos, sin, after)


def attn_kernel(n_tiles, parts, grp, bk, ext_step, hp, ck, info_ref, *refs):
    n_q = len(parts)
    q_refs, (k_ref, v_ref, _), o_refs = refs[:n_q], refs[n_q:n_q + 3], refs[n_q + 3:2 * n_q + 3]
    q_scr, s_scr, bm_scr, m_scr, l_scr, acc_scr = refs[2 * n_q + 3:]
    first_tile = parts[0][0]
    n = grp * T
    base = 2 * n_tiles + 3
    m_items = (info_ref.shape[0] - base) // 4

    def tile(i): return info_ref[base + i]

    def blk(i): return info_ref[base + m_items + i]

    def first(i): return info_ref[base + 2 * m_items + i]

    def diag(i): return info_ref[base + 3 * m_items + i]

    @pl.when((pl.program_id(0) == 0) & (pl.program_id(1) == 0))
    def _():
        l_scr[...] = jnp.zeros_like(l_scr)
        acc_scr[...] = jnp.zeros_like(acc_scr)
        m_scr[...] = jnp.zeros_like(m_scr)

    for h in range(hp):
        for (start, tiles), q_ref in zip(parts, q_refs):
            for t in range(tiles):
                for j in range(grp):
                    q_scr[h, start - first_tile + t, j * T:(j + 1) * T, :] = q_ref[0, t * T:(t + 1) * T, (h * grp + j) * HD:(h * grp + j + 1) * HD]

    def fold(x, op):
        return op(x.reshape(x.shape[0] // 8, 8, n), axis=0)

    def qk_chunk(i, h, r):
        s = lax.dot_general(k_ref[blk(i), r * ck:(r + 1) * ck, h * HD:(h + 1) * HD], q_scr[h, jnp.clip(tile(i) - first_tile, 0, q_scr.shape[1] - 1)], (((1,), (1,)), ((), ())), preferred_element_type=jnp.float32)
        s_scr[h, r * ck:(r + 1) * ck, :] = s
        return fold(s, jnp.max)

    def masked_chunk(i, h, r, ext):
        s = s_scr[h, r * ck:r * ck + ext, :]
        off = info_ref[n_tiles + tile(i)] - blk(i) * bk - r * ck
        row = lax.broadcasted_iota(jnp.int32, (ext, n), 0)
        col = lax.broadcasted_iota(jnp.int32, (ext, n), 1) & (T - 1)
        return jnp.where(row - col <= off, s, -jnp.inf)

    def body(i, ext, masked):
        b = blk(i)
        fresh = first(i) == 1
        for h in range(hp):
            if masked:
                bm = jnp.full((8, n), -jnp.inf, jnp.float32)
                for r in range(bk // ck):
                    e = min(ck, ext - r * ck)
                    if e <= 0:
                        continue
                    if r * ck + e > ext - ext_step:
                        sm = masked_chunk(i, h, r, e)
                        s_scr[h, r * ck:r * ck + e, :] = sm
                    else:
                        sm = s_scr[h, r * ck:r * ck + e, :]
                    bm = jnp.maximum(bm, fold(sm, jnp.max))
            else:
                bm = bm_scr[h]
            m_old = jnp.where(fresh, -jnp.inf, m_scr[h])
            m_new = jnp.maximum(m_old, jnp.max(bm, axis=0, keepdims=True))
            m_scr[h] = m_new
            alpha = jnp.exp2(m_old - m_new)
            l = l_scr[h] * alpha
            pv = None
            bm_next = None
            for r in range(bk // ck):
                e = min(ck, ext - r * ck)
                if e > 0:
                    p = jnp.exp2(s_scr[h, r * ck:r * ck + e, :] - m_new)
                    l = l + fold(p, jnp.sum)
                    d = jnp.dot(v_ref[b, h * HD:(h + 1) * HD, r * ck:r * ck + e], p.astype(jnp.bfloat16), preferred_element_type=jnp.float32)
                    pv = d if pv is None else pv + d
                x = qk_chunk(i + 1, h, r)
                bm_next = x if bm_next is None else jnp.maximum(bm_next, x)
            l_scr[h] = l
            bm_scr[h] = bm_next
            acc_scr[h] = acc_scr[h] * alpha + pv

    def finish(i):
        t = tile(i)
        for h in range(hp):
            inv = 1.0 / jnp.sum(l_scr[h], axis=0, keepdims=True)
            o = (acc_scr[h] * inv).T.astype(jnp.bfloat16)
            for (start, tiles), o_ref in zip(parts, o_refs):
                @pl.when((t >= start) & (t < start + tiles))
                def _():
                    at = pl.ds(pl.multiple_of((t - start) * T, T), T)
                    for j in range(grp):
                        o_ref[0, at, (h * grp + j) * HD:(h * grp + j + 1) * HD] = o[j * T:(j + 1) * T]

    begin = 0 if first_tile == 0 else info_ref[2 * n_tiles]
    end = info_ref[2 * n_tiles + (1 if n_q > 1 or first_tile else 0)]

    @pl.when(end > begin)
    def _():
        for h in range(hp):
            bm = None
            for r in range(bk // ck):
                x = qk_chunk(begin, h, r)
                bm = x if bm is None else jnp.maximum(bm, x)
            bm_scr[h] = bm

        def step(i, _):
            d = diag(i)

            @pl.when(d == 0)
            def _():
                body(i, bk, False)

            for e in range(bk // ext_step):
                @pl.when(d == e + 1)
                def _():
                    body(i, (e + 1) * ext_step, True)
                    finish(i)
            return 0

        lax.fori_loop(begin, end, step, 0)


def make_info(n_sp, seq_loc, moved, ext_step):
    n_tiles, spare = seq_loc // T, max(moved)
    rows = []
    for me in range(n_sp):
        other = n_sp - 1 - me
        pos = [me * seq_loc + t * T for t in range(n_tiles)]
        pos += [(other + 1) * seq_loc - (spare - t) * T for t in range(spare)]
        valid = [t < n_tiles - moved[me] for t in range(n_tiles)] + [t >= spare - moved[other] for t in range(spare)]
        items = []
        for t, p in enumerate(pos):
            if valid[t]:
                last = p // seq_loc
                for b in range(last + 1):
                    items.append((t, b, int(b == 0), (p - last * seq_loc) // ext_step + 1 if b == last else 0))
        own = sum(t < n_tiles for t, *_ in items)
        rows.append(([int(v) for v in valid] + pos + [own, len(items), moved[other]], items))
    m = max(len(items) for _, items in rows) + 1
    out = []
    for head, items in rows:
        items = items + [(0, 0, 0, 0)] * (m - len(items))
        out.append(head + [item[k] for k in range(4) for item in items])
    return np.asarray(out, np.int32)


def attention(qs, firsts, kv, info, after, first_prompt, n_kv, total_tiles, hp=4, ck=256):
    width = qs[0].shape[2]
    grp = width // HD // n_kv
    n_dev, nb, _, bk, _ = kv.shape
    parts = [(f, q.shape[1] // T) for f, q in zip(firsts, qs)]
    n_tiles = sum(t for _, t in parts)
    n = grp * T
    flops = 2 * 4 * nb * n_tiles * T * width * n_dev * bk // 2
    return pl.pallas_call(
        functools.partial(attn_kernel, total_tiles, parts, grp, bk, DIAG_STEP, hp, ck),
        out_shape=[jax.ShapeDtypeStruct((nb,) + q.shape[1:], q.dtype) for q in qs],
        grid_spec=pltpu.PrefetchScalarGridSpec(
            num_scalar_prefetch=1,
            grid=(nb, n_kv // hp),
            in_specs=[pl.BlockSpec((1, q.shape[1], hp * grp * HD), lambda p, h, *_: (p + first_prompt, 0, h)) for q in qs] + [
                pl.BlockSpec((n_dev, None, None, bk, hp * HD), lambda p, h, *_: (0, p, 0, 0, h)),
                pl.BlockSpec((n_dev, None, None, hp * HD, bk), lambda p, h, *_: (0, p, 1, h, 0)),
                pl.BlockSpec(memory_space=pl.ANY),
            ],
            out_specs=[pl.BlockSpec((1, q.shape[1], hp * grp * HD), lambda p, h, *_: (p, 0, h)) for q in qs],
            scratch_shapes=[
                pltpu.VMEM((hp, n_tiles, n, HD), qs[0].dtype),
                pltpu.VMEM((hp, bk, n), jnp.float32),
                pltpu.VMEM((hp, 8, n), jnp.float32),
                pltpu.VMEM((hp, 1, n), jnp.float32),
                pltpu.VMEM((hp, 8, n), jnp.float32),
                pltpu.VMEM((hp, HD, n), jnp.float32),
            ],
        ),
        compiler_params=pltpu.CompilerParams(dimension_semantics=("arbitrary", "arbitrary"), vmem_limit_bytes=VMEM_LIMIT),
        cost_estimate=pl.CostEstimate(flops=flops, bytes_accessed=4 * nb * n_tiles * T * width, transcendentals=0),
        name="attn",
    )(info, *qs, kv, kv, after)


def out_moved_kernel(taken, n_o, info_ref, *refs):
    o_refs, (w_ref, x_ref, y_ref) = refs[:n_o], refs[n_o:]

    @pl.when(info_ref[taken] > 0)
    def _():
        n_p, r, _ = x_ref.shape
        o = [o_ref[...].reshape(-1, o_ref.shape[2]) for o_ref in o_refs]
        y = jnp.dot(jnp.concatenate(o, axis=0), w_ref[...], preferred_element_type=jnp.float32)
        y_ref[...] = (x_ref[...].astype(jnp.float32) + y.reshape(n_p, r, -1)).astype(y_ref.dtype)


def out_moved(o_parts, w_out, x, info, first_prompt, total_tiles):
    _, rows, w = o_parts[0].shape
    nb = sum(o.shape[0] for o in o_parts)
    d = x.shape[2]
    nc = min(512, d)
    taken = 2 * total_tiles + 2
    col = lambda i, info: i * jnp.minimum(info[taken], 1)
    return pl.pallas_call(
        functools.partial(out_moved_kernel, taken, len(o_parts)),
        out_shape=jax.ShapeDtypeStruct((nb, rows, d), x.dtype),
        grid_spec=pltpu.PrefetchScalarGridSpec(
            num_scalar_prefetch=1,
            grid=(d // nc,),
            in_specs=[pl.BlockSpec(o.shape, lambda i, *_: (0, 0, 0)) for o in o_parts] + [
                pl.BlockSpec((w, nc), lambda i, info: (0, col(i, info))),
                pl.BlockSpec((pl.Element(nb), pl.Element(rows), pl.Element(nc)), lambda i, info: (first_prompt, 0, col(i, info) * nc)),
            ],
            out_specs=pl.BlockSpec((nb, rows, nc), lambda i, info: (0, 0, col(i, info))),
        ),
        compiler_params=pltpu.CompilerParams(dimension_semantics=("arbitrary",), vmem_limit_bytes=VMEM_LIMIT),
        cost_estimate=pl.CostEstimate(flops=2 * nb * rows * d * w, bytes_accessed=2 * w * d, transcendentals=0),
        name="out_moved",
    )(info, *o_parts, w_out, x)


def out_kernel(n_g, nc, info_ref, *refs):
    o_refs, (w_ref, x_ref, _, y_ref, o_scr, w_scr, sem) = refs[:n_g], refs[n_g:]
    i = pl.program_id(0)
    n_chunks = w_ref.shape[1] // nc

    def load(n):
        cols = slice(n * nc, (n + 1) * nc)
        return pltpu.make_async_copy(w_ref.at[:, cols], w_scr.at[:, cols], sem.at[n])

    @pl.when(i == 0)
    def _():
        for n in range(n_chunks):
            load(n).start()

    @pl.when(info_ref[i] == 1)
    def _():
        n_p, r, _ = x_ref.shape
        at = 0
        for o_ref in o_refs:
            nb, _, w = o_ref.shape
            o_scr[at:at + nb * r, :] = o_ref[...].reshape(nb * r, w)
            at += nb * r

        for n in range(n_chunks):
            @pl.when(i == 0)
            def _():
                load(n).wait()

            cols = slice(n * nc, (n + 1) * nc)
            y = jnp.dot(o_scr[...], w_scr[:, cols], preferred_element_type=jnp.float32)
            y_ref[:, :, cols] = (x_ref[:, :, cols].astype(jnp.float32) + y.reshape(n_p, r, nc)).astype(y_ref.dtype)


def out_local(o_parts, w_out, x, info, after):
    n_p, rows, d = x.shape
    w = o_parts[0].shape[2]
    n_g, nc = len(o_parts), min(1024, d)
    return pl.pallas_call(
        functools.partial(out_kernel, n_g, nc),
        out_shape=jax.ShapeDtypeStruct(x.shape, x.dtype),
        grid_spec=pltpu.PrefetchScalarGridSpec(
            num_scalar_prefetch=1,
            grid=(rows // T,),
            in_specs=[pl.BlockSpec((o.shape[0], T, w), lambda i, *_: (0, i, 0)) for o in o_parts] + [
                pl.BlockSpec(memory_space=pl.ANY),
                pl.BlockSpec((n_p, T, d), lambda i, *_: (0, i, 0)),
                pl.BlockSpec(memory_space=pl.ANY),
            ],
            out_specs=pl.BlockSpec((n_p, T, d), lambda i, *_: (0, i, 0)),
            scratch_shapes=[pltpu.VMEM((n_p * T, w), x.dtype), pltpu.VMEM((w, d), x.dtype), pltpu.SemaphoreType.DMA((d // nc,))],
        ),
        compiler_params=pltpu.CompilerParams(dimension_semantics=("arbitrary",), vmem_limit_bytes=VMEM_LIMIT),
        cost_estimate=pl.CostEstimate(flops=2 * n_p * rows * d * w, bytes_accessed=2 * n_p * rows * (d + w), transcendentals=0),
        name="out_local",
    )(info, *o_parts, w_out, x, after)


def merge_kernel(n_g, given_ref, *refs):
    y_refs, (cur_ref, out_ref) = refs[:n_g], refs[n_g:]

    @pl.when(given_ref[0] == 0)
    def _():
        out_ref[...] = cur_ref[...]

    @pl.when(given_ref[0] > 0)
    def _():
        at = 0
        for y_ref in y_refs:
            out_ref[at:at + y_ref.shape[0]] = y_ref[...]
            at += y_ref.shape[0]


def merge(returned, out, given):
    n_p, rows, d = out.shape
    back, n_tiles = returned[0].shape[1] // T, rows // T
    n_g = len(returned)
    at = lambda i, given: jnp.minimum(jnp.maximum(i, back - given[0]), back - 1)
    block = pl.BlockSpec((n_p, T, d), lambda i, given: (0, n_tiles - back + at(i, given), 0))
    return pl.pallas_call(
        functools.partial(merge_kernel, n_g),
        out_shape=jax.ShapeDtypeStruct(out.shape, out.dtype),
        grid_spec=pltpu.PrefetchScalarGridSpec(
            num_scalar_prefetch=1,
            grid=(back,),
            in_specs=[pl.BlockSpec((y.shape[0], T, d), lambda i, given: (0, at(i, given), 0)) for y in returned] + [block],
            out_specs=block,
        ),
        input_output_aliases={1 + n_g: 0},
        compiler_params=pltpu.CompilerParams(dimension_semantics=("arbitrary",), vmem_limit_bytes=VMEM_LIMIT),
        name="merge",
    )(given, *returned, out)


def rotary_tables(positions):
    half = HD // 2
    inv_freq = THETA ** (-jnp.arange(half, dtype=jnp.float32) * 2.0 / HD)
    angles = positions.astype(jnp.float32)[:, None] * inv_freq[None, :]
    cos, sin = jnp.cos(angles), jnp.sin(angles)
    return jnp.concatenate([cos, cos], axis=-1), jnp.concatenate([-sin, sin], axis=-1)


def solution(mesh):
    n_sp = mesh.shape["sp"]

    def block(tokens, w_query, w_key, w_value, w_out, attn_norm, q_norm, k_norm):
        n_p, seq_loc, _ = tokens.shape
        n_kv = w_key.shape[1] // HD
        n_tiles = seq_loc // T
        sizes = []
        while sum(sizes) < n_p:
            sizes.append(min(len(sizes) + 1, n_p - sum(sizes)))
        table = split_work(n_sp, n_tiles)
        spare = max(table)
        me = lax.axis_index("sp")
        gain, q_gain, k_gain = attn_norm.reshape(1, -1), q_norm.reshape(1, -1), k_norm.reshape(1, -1)

        away = [(d, n_sp - 1 - d) for d in range(n_sp) if table[d]]
        x_moved = lax.ppermute(tokens[:, seq_loc - spare * T:, :], "sp", away)

        starts = jnp.concatenate([
            me * seq_loc + jnp.arange(n_tiles) * T,
            (n_sp - me) * seq_loc - spare * T + jnp.arange(spare) * T,
        ])
        cos, sin = rotary_tables((starts[:, None] + jnp.arange(T)[None, :]).reshape(-1))
        info = jnp.asarray(make_info(n_sp, seq_loc, table, DIAG_STEP))[me]

        given = jnp.asarray(table, jnp.int32)[me].reshape(1)
        k, v, h, *packs = kv_project(tokens, w_key, w_value, gain, k_gain, cos, sin, sizes)
        kv = [lax.all_gather(pack, "sp") for pack in packs]
        total = n_tiles + spare
        q = q_project(h, w_query, gain, q_gain, cos, sin, info, 0, total, True, info)
        k, v, q = lax.optimization_barrier((k, v, q))
        own, extra, at = [], [], sizes[0]
        (o,) = attention([q], [0], kv[0], info, info, 0, n_kv, total)
        own.append(o)
        q_x = q_project(x_moved, w_query, gain, q_gain, cos, sin, info, n_tiles, total, False, o)
        (o_x,) = attention([q_x], [n_tiles], kv[0], info, info, 0, n_kv, total)
        extra.append(o_x)
        after, done, returned = o_x, 0, []
        for g in range(1, len(sizes)):
            o, o_x = attention([q, q_x], [0, n_tiles], kv[g], info, after, at, n_kv, total)
            at += sizes[g]
            own.append(o)
            extra.append(o_x)
            after = out_moved(extra, w_out, x_moved, info, done, total)
            returned.append(lax.ppermute(after, "sp", [(b, a) for a, b in away]))
            done, extra = at, []
        out = out_local(own, w_out, tokens, info, after)
        out = merge(returned, out, given)
        return out, k.reshape(n_p, seq_loc, n_kv, HD), v.reshape(n_p, seq_loc, n_kv, HD)

    rows, flat = P("dp", "sp", None), P(None, None)
    cache = P("dp", "sp", None, None)
    return jax.shard_map(
        block,
        mesh=mesh,
        in_specs=(rows, flat, flat, flat, flat, P(None), P(None), P(None)),
        out_specs=(rows, cache, cache),
        check_vma=False,
    )
```

```python
import functools
import math

import jax
import jax.numpy as jnp
import numpy as np
from jax import lax
from jax.experimental import pallas as pl
from jax.experimental.pallas import tpu as pltpu
from jax.sharding import PartitionSpec as P

EPS = 1e-6
THETA = 1000000.0
HD = 128
T = 64
VMEM_LIMIT = 60 * 1024 * 1024
Q_COLS = 512
DIAG_STEP = 256
TILE_COST, TAKEN_COST, ITEM_COST = 17.0, 25.0, 7.5


def split_work(n_sp, n_tiles):
    moved = [0] * n_sp
    for d in range((n_sp + 1) // 2, n_sp):
        low = n_sp - 1 - d
        high, small = ITEM_COST * (d + 1), ITEM_COST * (low + 1)
        moved[d] = min(
            range(n_tiles // 2 + 1),
            key=lambda k: max((n_tiles - k) * (TILE_COST + high), n_tiles * (TILE_COST + small) + k * (TAKEN_COST + high)),
        )
    return moved


def normed(x_ref, gain_ref):
    p, r, d = x_ref.shape
    x = x_ref[...].reshape(p * r, d).astype(jnp.float32)
    inv = lax.rsqrt(jnp.mean(x * x, axis=-1, keepdims=True) + EPS)
    return (x * inv * gain_ref[...].astype(jnp.float32)).astype(jnp.bfloat16)


def head_norm_rope(y, gain, cos, sin, n_rep):
    inv = lax.rsqrt(jnp.mean(y * y, axis=-1, keepdims=True) + EPS)
    y = y * inv * gain
    rolled = pltpu.roll(y, HD // 2, 1)
    r = cos.shape[0]
    y, rolled = y.reshape(n_rep, r, HD), rolled.reshape(n_rep, r, HD)
    return (y * cos[None] + rolled * sin[None]).astype(jnp.bfloat16)


def kv_kernel(sizes, x_ref, wk_ref, wv_ref, g_ref, kg_ref, cos_ref, sin_ref, *rest):
    k_ref, v_ref, h_ref, *pack_refs = rest[-3 - len(sizes):]
    n_p, r, d = x_ref.shape
    i = pl.program_id(0)
    h = normed(x_ref, g_ref)
    h_ref[...] = h.reshape(n_p, r, d)
    k = jnp.dot(h, wk_ref[...], preferred_element_type=jnp.float32).astype(jnp.bfloat16).astype(jnp.float32)
    v = jnp.dot(h, wv_ref[...], preferred_element_type=jnp.float32).astype(jnp.bfloat16)
    gain = kg_ref[...].astype(jnp.float32)
    cos, sin = cos_ref[...], sin_ref[...]
    rows = pl.ds(pl.multiple_of(i * r, r), r)
    v_ref[...] = v.reshape(v_ref.shape)
    at = 0
    for size, pack_ref in zip(sizes, pack_refs):
        for p in range(size):
            pack_ref[p, 1, :, rows] = v[(at + p) * r:(at + p + 1) * r].T
        at += size
    for j in range(k.shape[1] // HD):
        cols = slice(j * HD, (j + 1) * HD)
        y = head_norm_rope(k[:, cols], gain, cos, sin, n_p)
        k_ref[:, :, cols] = y
        at = 0
        for size, pack_ref in zip(sizes, pack_refs):
            pack_ref[:, 0, rows, cols] = y[at:at + size]
            at += size


def kv_project(x, w_key, w_value, gain, k_gain, cos, sin, sizes, first, into):
    n_p, rows, d = x.shape
    w = w_key.shape[1]
    n = sum(sizes)
    r = rows if n == 1 else min(128, rows)
    whole = lambda shape: pl.BlockSpec(shape, lambda i: (0,) * len(shape))
    cut = lambda cols: pl.BlockSpec((pl.Element(n), pl.Element(r), pl.Element(cols)), lambda i: (first, i * r, 0))
    packs = [(s, 2, rows, w) for s in sizes]
    return pl.pallas_call(
        functools.partial(kv_kernel, sizes),
        out_shape=[jax.ShapeDtypeStruct(s, x.dtype) for s in [(n_p, rows, w)] * 2 + [(n_p, rows, d)] + packs],
        grid=(rows // r,),
        in_specs=[
            cut(d), whole((d, w)), whole((d, w)), whole((1, d)), whole((1, HD)),
            pl.BlockSpec((r, HD), lambda i: (i, 0)), pl.BlockSpec((r, HD), lambda i: (i, 0)),
        ] + [pl.BlockSpec(memory_space=pl.ANY)] * len(into),
        out_specs=[cut(w), cut(w), cut(d)] + [whole(s) for s in packs],
        input_output_aliases={7 + i: i for i in range(len(into))},
        compiler_params=pltpu.CompilerParams(dimension_semantics=("arbitrary",), vmem_limit_bytes=VMEM_LIMIT),
        cost_estimate=pl.CostEstimate(flops=4 * n * rows * d * w, bytes_accessed=8 * n * rows * d, transcendentals=0),
        name="kv_proj",
    )(x, w_key, w_value, gain, k_gain, cos, sin, *into)


def q_kernel(nc, is_normed, step_of, info_ref, x_ref, w_ref, g_ref, qg_ref, cos_ref, sin_ref, after_ref, q_ref, h_scr, y_scr, w_scr, sem):
    n_p, r, d = x_ref.shape
    i = pl.program_id(0)
    begin, first_tile = step_of(info_ref)
    n_chunks = w_ref.shape[1] // nc

    def cols(n):
        return pl.ds(pl.multiple_of(n * nc, nc), nc)

    def load(n):
        return pltpu.make_async_copy(w_ref.at[:, cols(n)], w_scr.at[:, cols(n)], sem.at[n])

    @pl.when((info_ref[first_tile + i] == 1) & (i >= begin))
    def _():
        @pl.when(i == begin)
        def _():
            for n in range(n_chunks):
                load(n).start()

        h_scr[...] = x_ref[...].reshape(n_p * r, d) if is_normed else normed(x_ref, g_ref)
        gain = qg_ref[...].astype(jnp.float32) * (math.log2(math.e) / math.sqrt(HD))
        cos, sin = cos_ref[...], sin_ref[...]

        def arrived(n):
            @pl.when(i == begin)
            def _():
                load(n).wait()

        def project(n):
            y_scr[...] = jnp.dot(h_scr[...], w_scr[:, cols(n)], preferred_element_type=jnp.float32).astype(jnp.bfloat16)

        def finish(n):
            for j in range(nc // HD):
                y = head_norm_rope(y_scr[:, j * HD:(j + 1) * HD].astype(jnp.float32), gain, cos, sin, n_p)
                q_ref[:, 0, n * (nc // HD) + j] = y

        def step(n, _):
            arrived(n + 1)
            finish(n)
            project(n + 1)
            return 0

        arrived(0)
        project(0)
        lax.fori_loop(0, n_chunks - 1, step, 0)
        finish(n_chunks - 1)


def q_project(x, w_query, gain, q_gain, cos, sin, info, first_tile, total_tiles, is_normed, after):
    n_p, rows, d = x.shape
    w = w_query.shape[1]
    n_tiles = rows // T
    begin = lambda info: n_tiles - info[2 * total_tiles + 2] if first_tile else 0
    local = lambda i, info: jnp.minimum(jnp.maximum(i, begin(info)), n_tiles - 1)
    whole = lambda shape: pl.BlockSpec(shape, lambda i, info: (0,) * len(shape))
    table = pl.BlockSpec((T, HD), lambda i, info: (local(i, info) + first_tile, 0))
    nc = Q_COLS
    return pl.pallas_call(
        functools.partial(q_kernel, nc, is_normed, lambda info: (begin(info), first_tile)),
        out_shape=jax.ShapeDtypeStruct((n_p, n_tiles, w // HD, T, HD), x.dtype),
        grid_spec=pltpu.PrefetchScalarGridSpec(
            num_scalar_prefetch=1,
            grid=(n_tiles,),
            in_specs=[
                pl.BlockSpec((n_p, T, d), lambda i, info: (0, local(i, info), 0)),
                pl.BlockSpec(memory_space=pl.ANY),
                whole((1, d)), whole((1, HD)), table, table,
                pl.BlockSpec(memory_space=pl.ANY),
            ],
            out_specs=pl.BlockSpec((n_p, 1, w // HD, T, HD), lambda i, info: (0, local(i, info), 0, 0, 0)),
            scratch_shapes=[
                pltpu.VMEM((n_p * T, d), x.dtype), pltpu.VMEM((n_p * T, nc), x.dtype),
                pltpu.VMEM((d, w), x.dtype), pltpu.SemaphoreType.DMA((w // nc,)),
            ],
        ),
        compiler_params=pltpu.CompilerParams(dimension_semantics=("arbitrary",), vmem_limit_bytes=VMEM_LIMIT),
        cost_estimate=pl.CostEstimate(flops=2 * n_p * rows * d * w, bytes_accessed=2 * n_p * rows * (d + w), transcendentals=0),
        name="q_proj",
    )(info, x, w_query, gain, q_gain, cos, sin, after)


def attn_kernel(n_tiles, parts, grp, bk, ext_step, hp, ck, info_ref, *refs):
    n_q = len(parts)
    q_refs, (k_ref, v_ref, _), o_refs = refs[:n_q], refs[n_q:n_q + 3], refs[n_q + 3:2 * n_q + 3]
    s_scr, bm_scr, m_scr, l_scr, acc_scr, *q_scr = refs[2 * n_q + 3:]
    first_tile = parts[0][0]
    n = grp * T
    base = 2 * n_tiles + 3
    m_items = (info_ref.shape[0] - base) // 4

    def tile(i): return info_ref[base + i]

    def blk(i): return info_ref[base + m_items + i]

    def first(i): return info_ref[base + 2 * m_items + i]

    def diag(i): return info_ref[base + 3 * m_items + i]

    @pl.when((pl.program_id(0) == 0) & (pl.program_id(1) == 0))
    def _():
        l_scr[...] = jnp.zeros_like(l_scr)
        acc_scr[...] = jnp.zeros_like(acc_scr)
        m_scr[...] = jnp.zeros_like(m_scr)

    if n_q > 1:
        at = 0
        for (_, tiles), q_ref in zip(parts, q_refs):
            q_scr[0][at:at + tiles] = q_ref[0]
            at += tiles

    def q_rows(t, h):
        t = jnp.clip(t - first_tile, 0, sum(tiles for _, tiles in parts) - 1)
        src = q_scr[0].at[t] if n_q > 1 else q_refs[0].at[0, t]
        return src[h * grp:(h + 1) * grp].reshape(n, HD)

    def fold(x, op):
        return op(x.reshape(x.shape[0] // 8, 8, n), axis=0)

    def qk_chunk(i, h, r):
        s = lax.dot_general(k_ref[blk(i), r * ck:(r + 1) * ck, h * HD:(h + 1) * HD], q_rows(tile(i), h), (((1,), (1,)), ((), ())), preferred_element_type=jnp.float32)
        s_scr[h, r * ck:(r + 1) * ck, :] = s
        return fold(s, jnp.max)

    def masked_chunk(i, h, r, ext):
        s = s_scr[h, r * ck:r * ck + ext, :]
        off = info_ref[n_tiles + tile(i)] - blk(i) * bk - r * ck
        row = lax.broadcasted_iota(jnp.int32, (ext, n), 0)
        col = lax.broadcasted_iota(jnp.int32, (ext, n), 1) & (T - 1)
        return jnp.where(row - col <= off, s, -jnp.inf)

    def body(i, ext, masked):
        b = blk(i)
        fresh = first(i) == 1
        for h in range(hp):
            if masked:
                bm = jnp.full((8, n), -jnp.inf, jnp.float32)
                for r in range(bk // ck):
                    e = min(ck, ext - r * ck)
                    if e <= 0:
                        continue
                    if r * ck + e > ext - ext_step:
                        sm = masked_chunk(i, h, r, e)
                        s_scr[h, r * ck:r * ck + e, :] = sm
                    else:
                        sm = s_scr[h, r * ck:r * ck + e, :]
                    bm = jnp.maximum(bm, fold(sm, jnp.max))
            else:
                bm = bm_scr[h]
            m_old = jnp.where(fresh, -jnp.inf, m_scr[h])
            m_new = jnp.maximum(m_old, jnp.max(bm, axis=0, keepdims=True))
            m_scr[h] = m_new
            alpha = jnp.exp2(m_old - m_new)
            l = l_scr[h] * alpha
            pv = None
            bm_next = None
            for r in range(bk // ck):
                e = min(ck, ext - r * ck)
                if e > 0:
                    p = jnp.exp2(s_scr[h, r * ck:r * ck + e, :] - m_new)
                    l = l + fold(p, jnp.sum)
                    d = jnp.dot(v_ref[b, h * HD:(h + 1) * HD, r * ck:r * ck + e], p.astype(jnp.bfloat16), preferred_element_type=jnp.float32)
                    pv = d if pv is None else pv + d
                x = qk_chunk(i + 1, h, r)
                bm_next = x if bm_next is None else jnp.maximum(bm_next, x)
            l_scr[h] = l
            bm_scr[h] = bm_next
            acc_scr[h] = acc_scr[h] * alpha + pv

    def finish(i):
        t = tile(i)
        for h in range(hp):
            inv = 1.0 / jnp.sum(l_scr[h], axis=0, keepdims=True)
            o = (acc_scr[h] * inv).T.astype(jnp.bfloat16)
            for (start, tiles), o_ref in zip(parts, o_refs):
                @pl.when((t >= start) & (t < start + tiles))
                def _():
                    at = pl.ds(pl.multiple_of((t - start) * T, T), T)
                    for j in range(grp):
                        o_ref[0, at, (h * grp + j) * HD:(h * grp + j + 1) * HD] = o[j * T:(j + 1) * T]

    begin = 0 if first_tile == 0 else info_ref[2 * n_tiles]
    end = info_ref[2 * n_tiles + (1 if n_q > 1 or first_tile else 0)]

    @pl.when(end > begin)
    def _():
        for h in range(hp):
            bm = None
            for r in range(bk // ck):
                x = qk_chunk(begin, h, r)
                bm = x if bm is None else jnp.maximum(bm, x)
            bm_scr[h] = bm

        def step(i, _):
            d = diag(i)

            @pl.when(d == 0)
            def _():
                body(i, bk, False)

            for e in range(bk // ext_step):
                @pl.when(d == e + 1)
                def _():
                    body(i, (e + 1) * ext_step, True)
                    finish(i)
            return 0

        lax.fori_loop(begin, end, step, 0)


def make_info(n_sp, seq_loc, moved, ext_step):
    n_tiles, spare = seq_loc // T, max(moved)
    rows = []
    for me in range(n_sp):
        other = n_sp - 1 - me
        pos = [me * seq_loc + t * T for t in range(n_tiles)]
        pos += [(other + 1) * seq_loc - (spare - t) * T for t in range(spare)]
        valid = [t < n_tiles - moved[me] for t in range(n_tiles)] + [t >= spare - moved[other] for t in range(spare)]
        items = []
        for t, p in enumerate(pos):
            if valid[t]:
                last = p // seq_loc
                for b in range(last + 1):
                    items.append((t, b, int(b == 0), (p - last * seq_loc) // ext_step + 1 if b == last else 0))
        own = sum(t < n_tiles for t, *_ in items)
        rows.append(([int(v) for v in valid] + pos + [own, len(items), moved[other]], items))
    m = max(len(items) for _, items in rows) + 1
    out = []
    for head, items in rows:
        items = items + [(0, 0, 0, 0)] * (m - len(items))
        out.append(head + [item[k] for k in range(4) for item in items])
    return np.asarray(out, np.int32)


def attention(qs, firsts, kv, info, after, first_prompt, n_kv, total_tiles, hp=4, ck=256):
    heads = qs[0].shape[2]
    grp = heads // n_kv
    n_dev, nb, _, bk, _ = kv.shape
    parts = [(f, q.shape[1]) for f, q in zip(firsts, qs)]
    n_tiles = sum(t for _, t in parts)
    n = grp * T
    flops = 2 * 4 * nb * n_tiles * T * heads * HD * n_dev * bk // 2
    hh = hp * grp
    return pl.pallas_call(
        functools.partial(attn_kernel, total_tiles, parts, grp, bk, DIAG_STEP, hp, ck),
        out_shape=[jax.ShapeDtypeStruct((nb, t * T, heads * HD), qs[0].dtype) for _, t in parts],
        grid_spec=pltpu.PrefetchScalarGridSpec(
            num_scalar_prefetch=1,
            grid=(nb, n_kv // hp),
            in_specs=[pl.BlockSpec((1, t, hh, T, HD), lambda p, h, *_: (p + first_prompt, 0, h, 0, 0)) for _, t in parts] + [
                pl.BlockSpec((n_dev, None, None, bk, hp * HD), lambda p, h, *_: (0, p, 0, 0, h)),
                pl.BlockSpec((n_dev, None, None, hp * HD, bk), lambda p, h, *_: (0, p, 1, h, 0)),
                pl.BlockSpec(memory_space=pl.ANY),
            ],
            out_specs=[pl.BlockSpec((1, t * T, hh * HD), lambda p, h, *_: (p, 0, h)) for _, t in parts],
            scratch_shapes=[
                pltpu.VMEM((hp, bk, n), jnp.float32),
                pltpu.VMEM((hp, 8, n), jnp.float32),
                pltpu.VMEM((hp, 1, n), jnp.float32),
                pltpu.VMEM((hp, 8, n), jnp.float32),
                pltpu.VMEM((hp, HD, n), jnp.float32),
            ] + ([pltpu.VMEM((n_tiles, hh, T, HD), qs[0].dtype)] if len(qs) > 1 else []),
        ),
        compiler_params=pltpu.CompilerParams(dimension_semantics=("arbitrary", "arbitrary"), vmem_limit_bytes=VMEM_LIMIT),
        cost_estimate=pl.CostEstimate(flops=flops, bytes_accessed=4 * nb * n_tiles * T * heads * HD, transcendentals=0),
        name="attn",
    )(info, *qs, kv, kv, after)


def out_moved_kernel(taken, n_o, info_ref, *refs):
    o_refs, (w_ref, x_ref, y_ref) = refs[:n_o], refs[n_o:]

    @pl.when(info_ref[taken] > 0)
    def _():
        n_p, r, _ = x_ref.shape
        o = [o_ref[...].reshape(-1, o_ref.shape[2]) for o_ref in o_refs]
        y = jnp.dot(jnp.concatenate(o, axis=0), w_ref[...], preferred_element_type=jnp.float32)
        y_ref[...] = (x_ref[...].astype(jnp.float32) + y.reshape(n_p, r, -1)).astype(y_ref.dtype)


def out_moved(o_parts, w_out, x, info, first_prompt, total_tiles):
    _, rows, w = o_parts[0].shape
    nb = sum(o.shape[0] for o in o_parts)
    d = x.shape[2]
    nc = min(512, d)
    taken = 2 * total_tiles + 2
    col = lambda i, info: i * jnp.minimum(info[taken], 1)
    return pl.pallas_call(
        functools.partial(out_moved_kernel, taken, len(o_parts)),
        out_shape=jax.ShapeDtypeStruct((nb, rows, d), x.dtype),
        grid_spec=pltpu.PrefetchScalarGridSpec(
            num_scalar_prefetch=1,
            grid=(d // nc,),
            in_specs=[pl.BlockSpec(o.shape, lambda i, *_: (0, 0, 0)) for o in o_parts] + [
                pl.BlockSpec((w, nc), lambda i, info: (0, col(i, info))),
                pl.BlockSpec((pl.Element(nb), pl.Element(rows), pl.Element(nc)), lambda i, info: (first_prompt, 0, col(i, info) * nc)),
            ],
            out_specs=pl.BlockSpec((nb, rows, nc), lambda i, info: (0, 0, col(i, info))),
        ),
        compiler_params=pltpu.CompilerParams(dimension_semantics=("arbitrary",), vmem_limit_bytes=VMEM_LIMIT),
        cost_estimate=pl.CostEstimate(flops=2 * nb * rows * d * w, bytes_accessed=2 * w * d, transcendentals=0),
        name="out_moved",
    )(info, *o_parts, w_out, x)


def out_kernel(n_g, nc, info_ref, *refs):
    o_refs, (w_ref, x_ref, _, y_ref, o_scr, w_scr, sem) = refs[:n_g], refs[n_g:]
    i = pl.program_id(0)
    n_chunks = w_ref.shape[1] // nc

    def load(n):
        cols = slice(n * nc, (n + 1) * nc)
        return pltpu.make_async_copy(w_ref.at[:, cols], w_scr.at[:, cols], sem.at[n])

    @pl.when(i == 0)
    def _():
        for n in range(n_chunks):
            load(n).start()

    @pl.when(info_ref[i] == 1)
    def _():
        n_p, r, _ = x_ref.shape
        at = 0
        for o_ref in o_refs:
            nb, _, w = o_ref.shape
            o_scr[at:at + nb * r, :] = o_ref[...].reshape(nb * r, w)
            at += nb * r

        for n in range(n_chunks):
            @pl.when(i == 0)
            def _():
                load(n).wait()

            cols = slice(n * nc, (n + 1) * nc)
            y = jnp.dot(o_scr[...], w_scr[:, cols], preferred_element_type=jnp.float32)
            y_ref[:, :, cols] = (x_ref[:, :, cols].astype(jnp.float32) + y.reshape(n_p, r, nc)).astype(y_ref.dtype)


def out_local(o_parts, w_out, x, info, after):
    n_p, rows, d = x.shape
    w = o_parts[0].shape[2]
    n_g, nc = len(o_parts), min(1024, d)
    return pl.pallas_call(
        functools.partial(out_kernel, n_g, nc),
        out_shape=jax.ShapeDtypeStruct(x.shape, x.dtype),
        grid_spec=pltpu.PrefetchScalarGridSpec(
            num_scalar_prefetch=1,
            grid=(rows // T,),
            in_specs=[pl.BlockSpec((o.shape[0], T, w), lambda i, *_: (0, i, 0)) for o in o_parts] + [
                pl.BlockSpec(memory_space=pl.ANY),
                pl.BlockSpec((n_p, T, d), lambda i, *_: (0, i, 0)),
                pl.BlockSpec(memory_space=pl.ANY),
            ],
            out_specs=pl.BlockSpec((n_p, T, d), lambda i, *_: (0, i, 0)),
            scratch_shapes=[pltpu.VMEM((n_p * T, w), x.dtype), pltpu.VMEM((w, d), x.dtype), pltpu.SemaphoreType.DMA((d // nc,))],
        ),
        compiler_params=pltpu.CompilerParams(dimension_semantics=("arbitrary",), vmem_limit_bytes=VMEM_LIMIT),
        cost_estimate=pl.CostEstimate(flops=2 * n_p * rows * d * w, bytes_accessed=2 * n_p * rows * (d + w), transcendentals=0),
        name="out_local",
    )(info, *o_parts, w_out, x, after)


def merge_kernel(n_g, given_ref, *refs):
    y_refs, (cur_ref, out_ref) = refs[:n_g], refs[n_g:]

    @pl.when(given_ref[0] == 0)
    def _():
        out_ref[...] = cur_ref[...]

    @pl.when(given_ref[0] > 0)
    def _():
        at = 0
        for y_ref in y_refs:
            out_ref[at:at + y_ref.shape[0]] = y_ref[...]
            at += y_ref.shape[0]


def merge(returned, out, given):
    n_p, rows, d = out.shape
    back, n_tiles = returned[0].shape[1] // T, rows // T
    n_g = len(returned)
    at = lambda i, given: jnp.minimum(jnp.maximum(i, back - given[0]), back - 1)
    block = pl.BlockSpec((n_p, T, d), lambda i, given: (0, n_tiles - back + at(i, given), 0))
    return pl.pallas_call(
        functools.partial(merge_kernel, n_g),
        out_shape=jax.ShapeDtypeStruct(out.shape, out.dtype),
        grid_spec=pltpu.PrefetchScalarGridSpec(
            num_scalar_prefetch=1,
            grid=(back,),
            in_specs=[pl.BlockSpec((y.shape[0], T, d), lambda i, given: (0, at(i, given), 0)) for y in returned] + [block],
            out_specs=block,
        ),
        input_output_aliases={1 + n_g: 0},
        compiler_params=pltpu.CompilerParams(dimension_semantics=("arbitrary",), vmem_limit_bytes=VMEM_LIMIT),
        name="merge",
    )(given, *returned, out)


def rotary_tables(positions):
    half = HD // 2
    inv_freq = THETA ** (-jnp.arange(half, dtype=jnp.float32) * 2.0 / HD)
    angles = positions.astype(jnp.float32)[:, None] * inv_freq[None, :]
    cos, sin = jnp.cos(angles), jnp.sin(angles)
    return jnp.concatenate([cos, cos], axis=-1), jnp.concatenate([-sin, sin], axis=-1)


def solution(mesh):
    n_sp = mesh.shape["sp"]

    def block(tokens, w_query, w_key, w_value, w_out, attn_norm, q_norm, k_norm):
        n_p, seq_loc, _ = tokens.shape
        n_kv = w_key.shape[1] // HD
        n_tiles = seq_loc // T
        sizes = []
        while sum(sizes) < n_p:
            sizes.append(min(len(sizes) + 1, 2, n_p - sum(sizes)))
        table = split_work(n_sp, n_tiles)
        spare = max(table)
        me = lax.axis_index("sp")
        gain, q_gain, k_gain = attn_norm.reshape(1, -1), q_norm.reshape(1, -1), k_norm.reshape(1, -1)

        away = [(d, n_sp - 1 - d) for d in range(n_sp) if table[d]]
        x_moved = lax.ppermute(tokens[:, seq_loc - spare * T:, :], "sp", away)

        starts = jnp.concatenate([
            me * seq_loc + jnp.arange(n_tiles) * T,
            (n_sp - me) * seq_loc - spare * T + jnp.arange(spare) * T,
        ])
        cos, sin = rotary_tables((starts[:, None] + jnp.arange(T)[None, :]).reshape(-1))
        info = jnp.asarray(make_info(n_sp, seq_loc, table, DIAG_STEP))[me]

        given = jnp.asarray(table, jnp.int32)[me].reshape(1)
        *into, pack = kv_project(tokens, w_key, w_value, gain, k_gain, cos, sin, sizes[:1], 0, ())
        packs = [pack]
        if sizes[1:]:
            k, v, h, *more = kv_project(tokens, w_key, w_value, gain, k_gain, cos, sin, sizes[1:], sizes[0], into)
            packs += more
        else:
            k, v, h = into
        kv = [lax.all_gather(pack, "sp") for pack in packs]
        total = n_tiles + spare
        q = q_project(h, w_query, gain, q_gain, cos, sin, info, 0, total, True, info)
        k, v, q = lax.optimization_barrier((k, v, q))
        own, extra, at = [], [], sizes[0]
        (o,) = attention([q], [0], kv[0], info, info, 0, n_kv, total)
        own.append(o)
        q_x = q_project(x_moved, w_query, gain, q_gain, cos, sin, info, n_tiles, total, False, o)
        (o_x,) = attention([q_x], [n_tiles], kv[0], info, info, 0, n_kv, total)
        extra.append(o_x)
        after, done, returned = o_x, 0, []
        for g in range(1, len(sizes)):
            o, o_x = attention([q, q_x], [0, n_tiles], kv[g], info, after, at, n_kv, total)
            at += sizes[g]
            own.append(o)
            extra.append(o_x)
            after = o_x
            if 2 * (at - done) >= n_p or g == len(sizes) - 1:
                after = out_moved(extra, w_out, x_moved, info, done, total)
                returned.append(lax.ppermute(after, "sp", [(b, a) for a, b in away]))
                done, extra = at, []
        out = out_local(own, w_out, tokens, info, after)
        out = merge(returned, out, given)
        return out, k.reshape(n_p, seq_loc, n_kv, HD), v.reshape(n_p, seq_loc, n_kv, HD)

    rows, flat = P("dp", "sp", None), P(None, None)
    cache = P("dp", "sp", None, None)
    return jax.shard_map(
        block,
        mesh=mesh,
        in_specs=(rows, flat, flat, flat, flat, P(None), P(None), P(None)),
        out_specs=(rows, cache, cache),
        check_vma=False,
    )
```
